32 devices in a mesh: grp: 2 (over x), patch: 16 (over z, y, core).
Axes of the slice: x: 2, y: 2, z: 4, core: 2. Of those that a mesh axis runs over, the one named last changes fastest.
Arguments:
- features: bfloat16 [4, 16, 32, 640], P('grp', 'patch'), parts along dimension 0, may hold values from -6 to 6
- stale_conv_in: bfloat16 [4, 16, 32, 640], P('grp', 'patch'), parts along dimension 0, may hold values from -4.1875 to 4.1875
- stale_normed: bfloat16 [4, 16, 32, 640], P('grp', 'patch'), parts along dimension 0, may hold values from -6 to 6
- first_gain: float32 [640], replicated, may hold values from 0.1 to 1.9
- first_bias: float32 [640], replicated, may hold values from -1.8 to 1.8
- conv_weight: bfloat16 [3, 3, 640, 640], replicated, may hold values from -0.078125 to 0.078125
- conv_bias: float32 [640], replicated, may hold values from -1.8 to 1.8
- second_gain: float32 [640], replicated, may hold values from 0.1 to 1.9
- second_bias: float32 [640], replicated, may hold values from -1.8 to 1.8
- query_weight: bfloat16 [640, 640], replicated, may hold values from -6 to 6
- key_weight: bfloat16 [640, 640], replicated, may hold values from -6 to 6
- value_weight: bfloat16 [640, 640], replicated, may hold values from -0.25 to 0.25
- output_weight: bfloat16 [640, 640], replicated, may hold values from -0.25 to 0.25
- layer_gain: float32 [640], replicated, may hold values from 0.1 to 1.9
- cross_query: bfloat16 [640, 640], replicated, may hold values from -0.5 to 0.5
- cross_output: bfloat16 [640, 640], replicated, may hold values from -0.25 to 0.25
- text_keys: bfloat16 [4, 77, 640], P('grp'), parts along dimension 0, may hold values from -32 to 32
- text_values: bfloat16 [4, 77, 640], P('grp'), parts along dimension 0, may hold values from -6 to 6
Outputs:
- block_output: float32 [4, 16, 32, 640], P('grp', 'patch'), parts along dimension 0
The draws below stay inside these ranges and needn't reach their ends.
There are 2 independent parts, one for each index of `grp`. The reference program is written for one: setup_inputs(seed, part) draws one part's arguments, and reference() takes and returns one part's arrays. A program takes and returns all parts, laid end to end along the dimension named above; an argument that names none is the same for every part. Nothing has to cross between parts.
All inputs are finite; a program needn't handle non-finite values.
Results may differ from the reference program's by a relative error of at most 0.02.
The reference program's roundings to bfloat16 on the way count: a program that leaves them out, or rounds other values in their place, can miss the bound.
Values may be sent and summed in bfloat16 or wider, within the bound.
A program may use at most 128 MiB of HBM per device.

```python
import jax
import jax.numpy as jnp
from jax import lax

C = 640
GROUPS = 32
HEADS = 10
HEAD_DIM = 64
CTX = 77
HALF = 32
ATT = 640
IMAGES = 2
PATCHES = 16


def draw_features(key, part):
    key_noise = jax.random.fold_in(key, 11)
    key_channel = jax.random.fold_in(key, 12)
    place = jnp.arange(PATCHES, dtype=jnp.float32) / (PATCHES - 1)
    row_scale = (0.6 + 1.2 * place)[None, :, None, None]
    channel_scale = jax.random.uniform(key_channel, (1, 1, 1, C), jnp.float32, 0.5, 1.5)
    noise = jax.random.normal(key_noise, (IMAGES, PATCHES, HALF, C), jnp.float32)
    values = noise * row_scale * channel_scale
    return jnp.clip(values, -6.0, 6.0).astype(jnp.bfloat16)


def drawn_weight(key, salt, spread):
    key_noise = jax.random.fold_in(key, salt)
    values = jax.random.normal(key_noise, (C, ATT), jnp.float32) * spread
    return jnp.clip(values, -6.0, 6.0).astype(jnp.bfloat16)


def draw_query_weight(key, part):
    return drawn_weight(key, 81, (C // 9) ** (-0.5))


def draw_key_weight(key, part):
    return drawn_weight(key, 82, C ** (-0.5))


def draw_text_keys(key, part):
    key_noise = jax.random.fold_in(key, 91)
    values = jnp.clip(jax.random.normal(key_noise, (IMAGES, CTX, ATT), jnp.float32), -6.0, 6.0)
    return jnp.clip(values, -32.0, 32.0).astype(jnp.bfloat16)


def levels(own_key, shape, cuts, smallest, high):
    gain, own = 1.0, jax.random.fold_in(own_key, 6)
    for axis_at, blocks in cuts:
        draws = jnp.exp(jax.random.uniform(jax.random.fold_in(own, axis_at), (blocks,), jnp.float32, smallest / len(cuts), high / len(cuts)))
        gain = gain * jnp.repeat(draws, shape[axis_at] // blocks).reshape([-1 if axis == axis_at else 1 for axis in range(len(shape))])
    return gain


def gaussian(own_key, dims, scale, reach, shards=(), kind=jnp.bfloat16):
    factor_of = levels(own_key, dims, shards, -0.22, 0.18) if shards else 1.0
    array = jax.random.normal(own_key, dims, jnp.float32) * scale * factor_of
    return jnp.minimum(jnp.maximum(array, -reach), reach).astype(kind)


def setup_inputs(seed: int = 0, part: int = 0) -> dict:
    splits = jax.random.split(jax.random.key(seed), 19)
    part_keys = jax.random.split(jax.random.fold_in(splits[18], part), 19)
    return {
        "features": draw_features(jax.random.fold_in(jax.random.fold_in(splits[18], part), 71), part),
        "stale_conv_in": gaussian(part_keys[1], (IMAGES, PATCHES, HALF, C), 0.7, 4.1875, ((1, 16),)),
        "stale_normed": gaussian(part_keys[2], (IMAGES, PATCHES, HALF, C), 1.0, 6.0, ((1, 16),)),
        "first_gain": jnp.clip(1.0 + 0.18 * jax.random.normal(splits[3], (C,), jnp.float32), 0.1, 1.9),
        "first_bias": gaussian(splits[4], (C,), 0.3, 1.8, (), jnp.float32),
        "conv_weight": gaussian(splits[5], (3, 3, C, C), (9 * C) ** -0.5, 0.078125),
        "conv_bias": gaussian(splits[6], (C,), 0.3, 1.8, (), jnp.float32),
        "second_gain": jnp.clip(1.0 + 0.18 * jax.random.normal(splits[7], (C,), jnp.float32), 0.1, 1.9),
        "second_bias": gaussian(splits[8], (C,), 0.3, 1.8, (), jnp.float32),
        "query_weight": draw_query_weight(jax.random.fold_in(splits[18], 71), part),
        "key_weight": draw_key_weight(jax.random.fold_in(splits[18], 71), part),
        "value_weight": gaussian(splits[11], (C, ATT), C ** -0.5, 0.25),
        "output_weight": gaussian(splits[12], (ATT, C), ATT ** -0.5, 0.25),
        "layer_gain": jnp.clip(1.0 + 0.18 * jax.random.normal(splits[13], (C,), jnp.float32), 0.1, 1.9),
        "cross_query": gaussian(splits[14], (C, ATT), (C // 4) ** -0.5, 0.5),
        "cross_output": gaussian(splits[15], (ATT, C), ATT ** -0.5, 0.25),
        "text_keys": draw_text_keys(jax.random.fold_in(jax.random.fold_in(splits[18], part), 71), part),
        "text_values": gaussian(part_keys[17], (IMAGES, CTX, ATT), 1.0, 6.0),
    }


EPSILON = 1e-05

def narrow_exact(values):
    return lax.optimization_barrier(values.astype(jnp.bfloat16)).astype(jnp.float32)

def project(values, weight):
    return jnp.dot(values, weight, preferred_element_type=jnp.float32).astype(jnp.bfloat16)

def group_norm(features, scale_vec, shift_vec):
    images, patches, columns, channels = features.shape
    grouped = features.astype(jnp.float32).reshape(images, patches, columns, GROUPS, channels // GROUPS)
    group_mean = lax.optimization_barrier(jnp.mean(grouped, axis=(1, 2, 4), keepdims=True))
    group_var = lax.optimization_barrier(jnp.mean(jnp.square(grouped - group_mean), axis=(1, 2, 4), keepdims=True))
    normed = ((grouped - group_mean) * lax.rsqrt(group_var + EPSILON)).reshape(features.shape)
    return normed * scale_vec + shift_vec

def layer_norm(values, scale_vec):
    layer_mean = lax.optimization_barrier(jnp.mean(values, axis=-1, keepdims=True))
    centred = values - layer_mean
    layer_var = lax.optimization_barrier(jnp.mean(centred * centred, axis=-1, keepdims=True))
    return centred * lax.rsqrt(layer_var + EPSILON) * scale_vec

def patch_conv(fresh, stale, conv_weight):
    images = fresh.shape[0]
    row_count = PATCHES // 2
    image = stale.reshape(images, row_count, 2 * HALF, C)
    padded = jnp.pad(image, ((0, 0), (1, 1), (1, 1), (0, 0)))
    halves = []
    for half_side in range(2):
        columns_cut = padded[:, :, half_side * HALF:half_side * HALF + HALF + 2]
        halves.append(jnp.stack([columns_cut[:, offset:offset + row_count] for offset in range(3)], axis=2))
    windows = jnp.stack(halves, axis=2)
    centre = fresh.reshape(images, row_count, 2, HALF, C)
    windows = windows.at[:, :, :, 1, 1:HALF + 1].set(centre)
    total = jnp.zeros((images * row_count * 2 * HALF, C), jnp.float32)
    for offset_row in range(3):
        for offset_col in range(3):
            tap = windows[:, :, :, offset_row, offset_col:offset_col + HALF].reshape(-1, C)
            total = total + jnp.dot(tap, conv_weight[offset_row, offset_col], preferred_element_type=jnp.float32)
    return total.reshape(images, PATCHES, HALF, C)

def softmax_apply(queries, keys, values, scale):
    scores = jnp.einsum('bqhd,bkhd->bhqk', queries.astype(jnp.float32), keys.astype(jnp.float32)) * scale
    maxima = lax.optimization_barrier(jnp.max(scores, axis=-1, keepdims=True))
    weights = jnp.exp(scores - maxima)
    totals = lax.optimization_barrier(jnp.sum(weights, axis=-1))
    numer = jnp.einsum('bhqk,bkhd->bhqd', narrow_exact(weights), values.astype(jnp.float32))
    return numer / totals[..., None]

def reference(features, stale_conv_in, stale_normed, first_gain, first_bias, conv_weight, conv_bias, second_gain, second_bias, query_weight, key_weight, value_weight, output_weight, layer_gain, cross_query, cross_output, text_keys, text_values):
    images = features.shape[0]
    scale = HEAD_DIM ** (-0.5)
    conv_input = jax.nn.silu(group_norm(features, first_gain, first_bias)).astype(jnp.bfloat16)
    conv_out = patch_conv(conv_input, stale_conv_in, conv_weight)
    hidden = features.astype(jnp.float32) + conv_out + conv_bias
    attn_input = group_norm(hidden, second_gain, second_bias).astype(jnp.bfloat16)
    flat_input = attn_input.reshape(-1, C)
    stale_flat = stale_normed.reshape(-1, C)
    shape_att = (images, PATCHES, HALF, ATT)
    queries = project(flat_input, query_weight).reshape(shape_att)
    fresh_keys = project(flat_input, key_weight).reshape(shape_att)
    fresh_values = project(flat_input, value_weight).reshape(shape_att)
    stale_keys = project(stale_flat, key_weight).reshape(shape_att)
    stale_values = project(stale_flat, value_weight).reshape(shape_att)

    def one_patch(position):
        patch_queries = lax.dynamic_slice_in_dim(queries, position, 1, 1).reshape(images, HALF, HEADS, HEAD_DIM)
        own_keys = lax.dynamic_slice_in_dim(fresh_keys, position, 1, 1)
        own_values = lax.dynamic_slice_in_dim(fresh_values, position, 1, 1)
        keys_all = lax.dynamic_update_slice_in_dim(stale_keys, own_keys, position, 1).reshape(images, PATCHES * HALF, HEADS, HEAD_DIM)
        values_all = lax.dynamic_update_slice_in_dim(stale_values, own_values, position, 1).reshape(images, PATCHES * HALF, HEADS, HEAD_DIM)
        result = softmax_apply(patch_queries, keys_all, values_all, scale)
        return result.transpose(0, 2, 1, 3).reshape(images, HALF, ATT).astype(jnp.bfloat16)
    attended = lax.map(one_patch, jnp.arange(PATCHES, dtype=jnp.int32)).transpose(1, 0, 2, 3)
    mixed = hidden.reshape(-1, C) + jnp.dot(attended.reshape(-1, ATT), output_weight, preferred_element_type=jnp.float32)
    layer_in = layer_norm(mixed, layer_gain).astype(jnp.bfloat16)
    cross_q = project(layer_in, cross_query).reshape(images, PATCHES * HALF, HEADS, HEAD_DIM)
    text_k = text_keys.reshape(images, CTX, HEADS, HEAD_DIM)
    text_v = text_values.reshape(images, CTX, HEADS, HEAD_DIM)
    cross_result = softmax_apply(cross_q, text_k, text_v, scale)
    cross_attn = cross_result.transpose(0, 2, 1, 3).reshape(-1, ATT).astype(jnp.bfloat16)
    block_output = mixed + jnp.dot(cross_attn, cross_output, preferred_element_type=jnp.float32)
    return block_output.reshape(images, PATCHES, HALF, C)
```

```python
import functools

import jax
import jax.numpy as jnp
from jax import lax
from jax.experimental import pallas as pl
from jax.experimental.pallas import tpu as pltpu
from jax.sharding import PartitionSpec as P

GROUPS = 32
HEADS = 10
HEAD_DIM = 64
EPSILON = 1e-05
MESH = pl.DeviceIdType.MESH
LANES = 128
F32 = jnp.float32
BF16 = jnp.bfloat16
HIGH = lax.Precision.HIGHEST


def dot(a, b, **kw):
    return jnp.dot(a, b, preferred_element_type=F32, **kw)


def dot_t(a, b):
    return lax.dot_general(a, b, (((1,), (1,)), ((), ())), preferred_element_type=F32)


def group_matrix(channels, transposed):
    width = channels // GROUPS
    shape = (LANES, channels) if transposed else (channels, LANES)
    channel = lax.broadcasted_iota(jnp.int32, shape, 1 if transposed else 0)
    group = lax.broadcasted_iota(jnp.int32, shape, 0 if transposed else 1)
    inside = (channel >= group * width) & (channel < (group + 1) * width)
    return jnp.where(inside, 1.0, 0.0).astype(F32)


def pair_attention(q, k, v, lane):
    cols = q.shape[0]
    low = lane < HEAD_DIM
    both = jnp.concatenate([jnp.where(low, q, 0.0), jnp.where(low, 0.0, q)], axis=0).astype(BF16)
    scores = dot_t(both, k)
    weights = jnp.exp(scores - jnp.max(scores, axis=-1, keepdims=True))
    totals = jnp.sum(weights, axis=-1, keepdims=True)
    out = dot(weights.astype(BF16), v) / totals
    return jnp.where(low, out[:cols], out[cols:])


def kernel(
    patches, images, cols,
    feat_h, sconv_h, snorm_h, fg_h, fb_h, wc_h, cb_h, sg_h, sb_h,
    wq_h, wk_h, wv_h, wo_h, lg_h, wcq_h, wco_h, tk_h, tv_h,
    out_ref,
    feat, sconv, xall, kall, vall, wc, ws, vec, tk, tv,
    stats, halo, edge_src, edges, lhs, hid, att,
    st_send, st_recv, xz_send, xy_send, xc_send, x_recv,
    halo_send, halo_recv, edge_send, edge_recv, in_sem, wc_sem, w_sem, v_sem,
):
    channels = feat.shape[-1]
    rows = images * cols
    outer = patches // 4
    chips = patches // 2
    me = lax.axis_index("patch")
    chip, core = me // 2, me % 2
    zo, yi = chip // 2, chip % 2
    partner = chip * 2 + (1 - core)

    def index(o, i, c):
        return (o * 2 + i) * 2 + c

    def xslot(slot):
        return xall.at[:, pl.ds(pl.multiple_of(slot * cols, cols), cols), :]

    cp_feat = pltpu.make_async_copy(feat_h, feat, in_sem.at[0])
    cp_sconv = pltpu.make_async_copy(sconv_h, sconv, in_sem.at[1])
    cp_snorm = pltpu.make_async_copy(snorm_h, xslot(me), in_sem.at[2])
    cp_tk = pltpu.make_async_copy(tk_h, tk, in_sem.at[3])
    cp_tv = pltpu.make_async_copy(tv_h, tv, in_sem.at[4])
    cp_feat.start()
    cp_sconv.start()
    cp_snorm.start()
    cp_vec = [
        pltpu.make_async_copy(h, vec.at[t], v_sem.at[t])
        for t, h in enumerate((fg_h, fb_h, cb_h, sg_h, sb_h, lg_h))
    ]
    for c in cp_vec:
        c.start()
    barrier = pltpu.get_barrier_semaphore()

    def greet(d, carry):
        pl.semaphore_signal(
            barrier, inc=1, device_id={"patch": lax.rem(me + d, patches)}, device_id_type=MESH
        )
        return carry

    row_first, row_last = chip == 0, chip == chips - 1

    @pl.when(row_first)
    def _():
        halo[0] = jnp.zeros(halo.shape[1:], BF16)
        edges[0] = jnp.zeros(edges.shape[1:], F32)

    @pl.when(row_last)
    def _():
        halo[1] = jnp.zeros(halo.shape[1:], BF16)
        edges[2] = jnp.zeros(edges.shape[1:], F32)

    lax.fori_loop(1, patches, greet, 0)
    cp_wc = {}
    for j in range(3):
        for i in range(3):
            cp_wc[i, j] = pltpu.make_async_copy(wc_h.at[i, j], wc.at[i, j], wc_sem.at[i * 3 + j])
            cp_wc[i, j].start()
    cp_w = [
        pltpu.make_async_copy(h, ws.at[t], w_sem.at[t])
        for t, h in enumerate((wk_h, wv_h, wq_h, wo_h, wcq_h, wco_h))
    ]
    for c in cp_w:
        c.start()
    cp_tk.start()
    cp_tv.start()

    gather_groups = group_matrix(channels, False)
    spread_groups = group_matrix(channels, True)
    count = float(patches * cols * (channels // GROUPS))

    def local_stats(phase, x):
        sums = [jnp.sum(x[b * cols:(b + 1) * cols], axis=0, keepdims=True) for b in range(images)]
        squares = [
            jnp.sum(x[b * cols:(b + 1) * cols] * x[b * cols:(b + 1) * cols], axis=0, keepdims=True)
            for b in range(images)
        ]
        table = jnp.concatenate(sums + squares, axis=0)
        stats[phase, me] = dot(table, gather_groups, precision=HIGH)

    def stat_copy(phase, slot, d):
        return pltpu.make_async_remote_copy(
            src_ref=stats.at[phase, slot],
            dst_ref=stats.at[phase, slot],
            send_sem=st_send.at[phase, d],
            recv_sem=st_recv.at[phase, slot],
            device_id={"patch": lax.rem(me + d, patches)},
            device_id_type=MESH,
        )

    def send_stats(phase):
        def body(d, carry):
            stat_copy(phase, me, d).start()
            return carry
        lax.fori_loop(1, patches, body, 0)

    def finish_stats(phase):
        def body(d, carry):
            stat_copy(phase, lax.rem(me + d, patches), d).wait_recv()
            return carry
        lax.fori_loop(1, patches, body, 0)
        total = jnp.sum(stats[phase], axis=0) / count
        mean = total[:images]
        var = total[images:] - mean * mean
        table = jnp.concatenate([mean, lax.rsqrt(var + EPSILON)], axis=0)
        return dot(table, spread_groups, precision=HIGH)

    def normed(x, table, b, gain, bias):
        part = x[b * cols:(b + 1) * cols]
        return (part - table[b:b + 1]) * table[images + b:images + b + 1] * gain + bias

    def x_copy(slot, target, send):
        return pltpu.make_async_remote_copy(
            src_ref=xslot(slot), dst_ref=xslot(slot), send_sem=send, recv_sem=x_recv.at[slot],
            device_id={"patch": target}, device_id_type=MESH,
        )

    def halo_copy(which, step):
        return pltpu.make_async_remote_copy(
            src_ref=sconv, dst_ref=halo.at[which], send_sem=halo_send.at[which],
            recv_sem=halo_recv.at[which],
            device_id={"patch": lax.rem(me + 2 * step + patches, patches)}, device_id_type=MESH,
        )

    def edge_copy(which, step):
        return pltpu.make_async_remote_copy(
            src_ref=edge_src, dst_ref=edges.at[which], send_sem=edge_send.at[which],
            recv_sem=edge_recv.at[which],
            device_id={"patch": lax.rem(partner + 2 * step + patches, patches)}, device_id_type=MESH,
        )

    cp_feat.wait()
    x = feat[...].reshape(rows, channels).astype(F32)
    local_stats(0, x)
    cp_sconv.wait()
    whole_conv = sconv[...].astype(F32)
    edge_src[...] = jnp.where(core == 0, whole_conv[:, cols - 1], whole_conv[:, 0])
    for c in cp_vec:
        c.wait()
    cp_snorm.wait()

    pl.semaphore_wait(barrier, patches - 1)
    send_stats(0)
    edge_copy(1, 0).start()

    @pl.when(jnp.logical_not(row_last))
    def _():
        halo_copy(0, 1).start()
        edge_copy(0, 1).start()

    @pl.when(jnp.logical_not(row_first))
    def _():
        halo_copy(1, -1).start()
        edge_copy(2, -1).start()

    x_copy(me, index(zo, 1 - yi, core), xy_send.at[0]).start()

    def z_send(d, carry):
        x_copy(me, index(lax.rem(zo + d, outer), yi, core), xz_send.at[d]).start()
        return carry

    lax.fori_loop(1, outer, z_send, 0)
    x_copy(me, partner, xc_send.at[0]).start()

    def forward_z(d, carry):
        slot = index(lax.rem(zo - d + outer, outer), yi, core)
        x_copy(slot, partner, xz_send.at[d]).wait_recv()
        x_copy(slot, index(zo, 1 - yi, core), xy_send.at[d]).start()
        x_copy(slot, partner, xc_send.at[d]).start()
        return carry

    def forward_y(d, carry):
        slot = index(lax.rem(zo - d + outer, outer), 1 - yi, core)
        x_copy(slot, partner, xz_send.at[0]).wait_recv()
        x_copy(slot, partner, xc_send.at[outer + d]).start()
        return carry

    table = finish_stats(0)
    for b in range(images):
        v = normed(x, table, b, vec[0], vec[1])
        lhs[1, b * cols:(b + 1) * cols, :] = (v * (1.0 / (1.0 + jnp.exp(-v)))).astype(BF16)

    edge_copy(1, 0).wait_recv()

    @pl.when(jnp.logical_not(row_first))
    def _():
        halo_copy(0, 1).wait_recv()
        edge_copy(0, 1).wait_recv()

    @pl.when(jnp.logical_not(row_last))
    def _():
        halo_copy(1, -1).wait_recv()
        edge_copy(2, -1).wait_recv()

    for which, row in ((0, 0), (1, 2)):
        lhs[row, :rows, :] = halo[which].reshape(rows, channels)
    filler = jnp.zeros((lhs.shape[1] - rows - images, channels), F32)
    for row in range(3):
        lhs[row, rows:, :] = jnp.concatenate([edges[row], filler], axis=0).astype(BF16)

    third = [1 + (outer - 1) * t // 3 for t in range(4)]
    parts = []
    for j in range(3):
        total = None
        for i in range(3):
            cp_wc[i, j].wait()
            term = dot(lhs[i], wc[i, j])
            total = term if total is None else total + term
        parts.append(total)
        if j < 2:
            lax.fori_loop(third[j], third[j + 1], forward_z, 0)
    place = lax.broadcasted_iota(jnp.int32, (cols, channels), 0)
    for b in range(images):
        left = pltpu.roll(parts[0][b * cols:(b + 1) * cols], 1, 0)
        right = pltpu.roll(parts[2][b * cols:(b + 1) * cols], cols - 1, 0)
        left_edge = jnp.where(core == 1, parts[0][rows + b:rows + b + 1], 0.0)
        right_edge = jnp.where(core == 0, parts[2][rows + b:rows + b + 1], 0.0)
        left = jnp.where(place == 0, left_edge, left)
        right = jnp.where(place == cols - 1, right_edge, right)
        conv = left + parts[1][b * cols:(b + 1) * cols] + right
        hid[b * cols:(b + 1) * cols, :] = x[b * cols:(b + 1) * cols] + conv + vec[2]

    hidden = hid[...]
    local_stats(1, hidden)
    send_stats(1)
    lax.fori_loop(third[2], third[3], forward_z, 0)
    lax.fori_loop(0, outer, forward_y, 0)

    def from_partner(t, carry):
        x_copy(t * 2 + (1 - core), partner, xz_send.at[0]).wait_recv()
        return carry

    lax.fori_loop(0, chips, from_partner, 0)
    cp_w[0].wait()
    cp_w[1].wait()
    span = patches * cols
    piece = min(span, 256)

    def stale_kv(t, carry):
        at = pl.ds(pl.multiple_of(t * piece, piece), piece)
        for b in range(images):
            block = xall[b, at, :]
            kall[b, at, :] = dot(block, ws[0]).astype(BF16)
            vall[b, at, :] = dot(block, ws[1]).astype(BF16)
        return carry

    lax.fori_loop(0, span // piece, stale_kv, 0)
    cp_w[2].wait()
    table = finish_stats(1)
    attn_in = jnp.concatenate(
        [normed(hidden, table, b, vec[3], vec[4]) for b in range(images)], axis=0
    ).astype(BF16)
    own = pl.ds(pl.multiple_of(me * cols, cols), cols)
    fresh_k = dot(attn_in, ws[0]).astype(BF16)
    fresh_v = dot(attn_in, ws[1]).astype(BF16)
    for b in range(images):
        kall[b, own, :] = fresh_k[b * cols:(b + 1) * cols]
        vall[b, own, :] = fresh_v[b * cols:(b + 1) * cols]
    scale = HEAD_DIM ** -0.5
    lane = lax.broadcasted_iota(jnp.int32, (cols, LANES), 1)

    def heads(q, keys, values):
        for b in range(images):
            for pair in range(channels // LANES):
                at = slice(pair * LANES, (pair + 1) * LANES)
                part = pair_attention(
                    q[b * cols:(b + 1) * cols, at], keys[b, :, at], values[b, :, at], lane
                )
                att[b * cols:(b + 1) * cols, at] = part.astype(BF16)

    heads(dot(attn_in, ws[2]).astype(BF16).astype(F32) * scale, kall, vall)
    cp_w[3].wait()
    mixed = hidden + dot(att[...], ws[3])
    centred = mixed - jnp.mean(mixed, axis=-1, keepdims=True)
    variance = jnp.mean(centred * centred, axis=-1, keepdims=True)
    layer_in = (centred * lax.rsqrt(variance + EPSILON) * vec[5]).astype(BF16)
    cp_w[4].wait()
    cp_tk.wait()
    cp_tv.wait()
    heads(dot(layer_in, ws[4]).astype(BF16).astype(F32) * scale, tk, tv)
    cp_w[5].wait()
    out_ref[...] = (mixed + dot(att[...], ws[5])).reshape(images, 1, cols, channels)

    def drain_stats(d, carry):
        stat_copy(0, me, d).wait_send()
        stat_copy(1, me, d).wait_send()
        return carry

    lax.fori_loop(1, patches, drain_stats, 0)

    def drain_z(d, carry):
        x_copy(me, partner, xz_send.at[d]).wait_send()
        return carry

    lax.fori_loop(1, outer, drain_z, 0)

    def drain_y(d, carry):
        x_copy(me, partner, xy_send.at[d]).wait_send()
        return carry

    lax.fori_loop(0, outer, drain_y, 0)

    def drain_c(d, carry):
        x_copy(me, partner, xc_send.at[d]).wait_send()
        return carry

    lax.fori_loop(0, chips, drain_c, 0)
    edge_copy(1, 0).wait_send()

    @pl.when(jnp.logical_not(row_last))
    def _():
        halo_copy(0, 1).wait_send()
        edge_copy(0, 1).wait_send()

    @pl.when(jnp.logical_not(row_first))
    def _():
        halo_copy(1, -1).wait_send()
        edge_copy(2, -1).wait_send()


def solution(mesh):
    patches = mesh.shape["patch"]

    def on_device(
        features, stale_conv_in, stale_normed, first_gain, first_bias, conv_weight, conv_bias,
        second_gain, second_bias, query_weight, key_weight, value_weight, output_weight,
        layer_gain, cross_query, cross_output, text_keys, text_values,
    ):
        images, _, cols, channels = features.shape
        rows = images * cols
        span = patches * cols
        outer = patches // 4

        def flat(a):
            return a.reshape(images, cols, channels)

        def row(a):
            return a.reshape(1, channels)

        dma = pltpu.SemaphoreType.DMA
        return pl.pallas_call(
            functools.partial(kernel, patches, images, cols),
            out_shape=jax.ShapeDtypeStruct(features.shape, F32),
            in_specs=[pl.BlockSpec(memory_space=pl.ANY)] * 18,
            out_specs=pl.BlockSpec(memory_space=pltpu.VMEM),
            scratch_shapes=[
                pltpu.VMEM((images, cols, channels), BF16),
                pltpu.VMEM((images, cols, channels), BF16),
                pltpu.VMEM((images, span, channels), BF16),
                pltpu.VMEM((images, span, channels), BF16),
                pltpu.VMEM((images, span, channels), BF16),
                pltpu.VMEM(conv_weight.shape, BF16),
                pltpu.VMEM((6, channels, channels), BF16),
                pltpu.VMEM((6, 1, channels), F32),
                pltpu.VMEM(text_keys.shape, BF16),
                pltpu.VMEM(text_values.shape, BF16),
                pltpu.VMEM((2, patches, 2 * images, LANES), F32),
                pltpu.VMEM((2, images, cols, channels), BF16),
                pltpu.VMEM((images, channels), F32),
                pltpu.VMEM((3, images, channels), F32),
                pltpu.VMEM((3, rows + 16, channels), BF16),
                pltpu.VMEM((rows, channels), F32),
                pltpu.VMEM((rows, channels), BF16),
                dma((2, patches)), dma((2, patches)),
                dma((outer,)), dma((outer,)), dma((2 * outer,)), dma((patches,)),
                dma((2,)), dma((2,)), dma((3,)), dma((3,)),
                dma((5,)), dma((9,)), dma((6,)), dma((6,)),
            ],
            compiler_params=pltpu.CompilerParams(
                collective_id=0, has_side_effects=True, vmem_limit_bytes=63000 * 1024
            ),
        )(
            flat(features), flat(stale_conv_in), flat(stale_normed), row(first_gain),
            row(first_bias), conv_weight, row(conv_bias), row(second_gain), row(second_bias),
            query_weight, key_weight, value_weight, output_weight, row(layer_gain),
            cross_query, cross_output, text_keys, text_values,
        )

    act = P("grp", "patch", None, None)
    text = P("grp", None, None)
    return jax.shard_map(
        on_device, mesh=mesh,
        in_specs=(act,) * 3 + (P(),) * 13 + (text,) * 2,
        out_specs=act, check_vma=False,
    )
```

```python
import functools

import jax
import jax.numpy as jnp
from jax import lax
from jax.experimental import pallas as pl
from jax.experimental.pallas import tpu as pltpu
from jax.sharding import PartitionSpec as P

GROUPS = 32
HEADS = 10
HEAD_DIM = 64
EPSILON = 1e-05
MESH = pl.DeviceIdType.MESH
LANES = 128
F32 = jnp.float32
BF16 = jnp.bfloat16
HIGH = lax.Precision.HIGHEST


def mark(name):
    pass


def dot(a, b, **kw):
    return jnp.dot(a, b, preferred_element_type=F32, **kw)


def dot_t(a, b):
    return lax.dot_general(a, b, (((1,), (1,)), ((), ())), preferred_element_type=F32)


def group_matrix(channels, transposed):
    width = channels // GROUPS
    shape = (LANES, channels) if transposed else (channels, LANES)
    channel = lax.broadcasted_iota(jnp.int32, shape, 1 if transposed else 0)
    group = lax.broadcasted_iota(jnp.int32, shape, 0 if transposed else 1)
    inside = (channel >= group * width) & (channel < (group + 1) * width)
    return jnp.where(inside, 1.0, 0.0).astype(F32)


def pair_attention(q, k, v, lane):
    cols = q.shape[0]
    low = lane < HEAD_DIM
    both = jnp.concatenate([jnp.where(low, q, 0.0), jnp.where(low, 0.0, q)], axis=0).astype(BF16)
    scores = dot_t(both, k)
    weights = jnp.exp(scores - jnp.max(scores, axis=-1, keepdims=True))
    totals = jnp.sum(weights, axis=-1, keepdims=True)
    out = dot(weights.astype(BF16), v) / totals
    return jnp.where(low, out[:cols], out[cols:])


def kernel(
    patches, images, cols,
    feat_h, sconv_h, snorm_h, fg_h, fb_h, wc_h, cb_h, sg_h, sb_h,
    wq_h, wk_h, wv_h, wo_h, lg_h, wcq_h, tk_h, tv_h,
    mixed_ref, att_ref,
    feat, sconv, xall, kall, vall, wc, ws, v0, v1, v2, v3, v4, v5, tk_in, tv_in, tk, tv,
    stats, halo, edge_src, edges, lhs, hid, att,
    st_send, st_recv, xz_send, xy_send, xc_send, x_recv,
    halo_send, halo_recv, edge_send, edge_recv, in_sem, wc_sem, w_sem, v_sem,
):
    channels = feat.shape[-1]
    rows = images * cols
    outer = patches // 4
    chips = patches // 2
    me = lax.axis_index("patch")
    chip, core = me // 2, me % 2
    zo, yi = chip // 2, chip % 2
    partner = chip * 2 + (1 - core)

    def index(o, i, c):
        return (o * 2 + i) * 2 + c

    def xslot(slot):
        return xall.at[:, pl.ds(pl.multiple_of(slot * cols, cols), cols), :]

    cp_feat = pltpu.make_async_copy(feat_h, feat, in_sem.at[0])
    cp_sconv = pltpu.make_async_copy(sconv_h, sconv, in_sem.at[1])
    cp_snorm = pltpu.make_async_copy(snorm_h, xslot(me), in_sem.at[2])
    cp_tk = pltpu.make_async_copy(tk_h, tk_in, in_sem.at[3])
    cp_tv = pltpu.make_async_copy(tv_h, tv_in, in_sem.at[4])
    cp_feat.start()
    cp_sconv.start()
    cp_snorm.start()
    cp_vec = [
        pltpu.make_async_copy(h, own_vec, v_sem.at[t])
        for t, (h, own_vec) in enumerate(zip((fg_h, fb_h, cb_h, sg_h, sb_h, lg_h), (v0, v1, v2, v3, v4, v5)))
    ]
    for c in cp_vec:
        c.start()
    barrier = pltpu.get_barrier_semaphore()

    def greet(d, carry):
        pl.semaphore_signal(
            barrier, inc=1, device_id={"patch": lax.rem(me + d, patches)}, device_id_type=MESH
        )
        return carry

    row_first, row_last = chip == 0, chip == chips - 1

    @pl.when(row_first)
    def _():
        halo[0] = jnp.zeros(halo.shape[1:], BF16)
        edges[0] = jnp.zeros(edges.shape[1:], F32)

    @pl.when(row_last)
    def _():
        halo[1] = jnp.zeros(halo.shape[1:], BF16)
        edges[2] = jnp.zeros(edges.shape[1:], F32)

    lax.fori_loop(1, patches, greet, 0)
    cp_wc = {}
    for j in range(3):
        for i in range(3):
            cp_wc[i, j] = pltpu.make_async_copy(wc_h.at[i, j], wc.at[i, j], wc_sem.at[i * 3 + j])
            cp_wc[i, j].start()
    cp_w = [
        pltpu.make_async_copy(h, ws.at[t], w_sem.at[t])
        for t, h in enumerate((wk_h, wv_h, wq_h, wo_h, wcq_h))
    ]
    for c in cp_w:
        c.start()
    cp_tk.start()
    cp_tv.start()

    gather_groups = group_matrix(channels, False)
    spread_groups = group_matrix(channels, True)
    count = float(patches * cols * (channels // GROUPS))

    def local_stats(phase, x):
        sums = [jnp.sum(x[b * cols:(b + 1) * cols], axis=0, keepdims=True) for b in range(images)]
        squares = [
            jnp.sum(x[b * cols:(b + 1) * cols] * x[b * cols:(b + 1) * cols], axis=0, keepdims=True)
            for b in range(images)
        ]
        table = jnp.concatenate(sums + squares, axis=0)
        stats[phase, me] = dot(table, gather_groups, precision=HIGH)

    def stat_copy(phase, slot, d):
        return pltpu.make_async_remote_copy(
            src_ref=stats.at[phase, slot],
            dst_ref=stats.at[phase, slot],
            send_sem=st_send.at[phase, d],
            recv_sem=st_recv.at[phase, slot],
            device_id={"patch": lax.rem(me + d, patches)},
            device_id_type=MESH,
        )

    def send_stats(phase):
        def body(d, carry):
            stat_copy(phase, me, d).start()
            return carry
        lax.fori_loop(1, patches, body, 0)

    def finish_stats(phase):
        def body(d, carry):
            stat_copy(phase, lax.rem(me + d, patches), d).wait_recv()
            return carry
        lax.fori_loop(1, patches, body, 0)
        total = jnp.sum(stats[phase], axis=0) / count
        mean = total[:images]
        var = total[images:] - mean * mean
        table = jnp.concatenate([mean, lax.rsqrt(var + EPSILON)], axis=0)
        return dot(table, spread_groups, precision=HIGH)

    def normed(x, table, b, gain, bias):
        part = x[b * cols:(b + 1) * cols]
        return (part - table[b:b + 1]) * table[images + b:images + b + 1] * gain + bias

    def x_copy(slot, target, send):
        return pltpu.make_async_remote_copy(
            src_ref=xslot(slot), dst_ref=xslot(slot), send_sem=send, recv_sem=x_recv.at[slot],
            device_id={"patch": target}, device_id_type=MESH,
        )

    def halo_copy(which, step):
        return pltpu.make_async_remote_copy(
            src_ref=sconv, dst_ref=halo.at[which], send_sem=halo_send.at[which],
            recv_sem=halo_recv.at[which],
            device_id={"patch": lax.rem(me + 2 * step + patches, patches)}, device_id_type=MESH,
        )

    def edge_copy(which, step):
        return pltpu.make_async_remote_copy(
            src_ref=edge_src, dst_ref=edges.at[which], send_sem=edge_send.at[which],
            recv_sem=edge_recv.at[which],
            device_id={"patch": lax.rem(partner + 2 * step + patches, patches)}, device_id_type=MESH,
        )

    mark("stats0")
    cp_feat.wait()
    x = feat[...].reshape(rows, channels).astype(F32)
    local_stats(0, x)
    mark("edges")
    cp_sconv.wait()
    whole_conv = sconv[...].astype(F32)
    edge_src[...] = jnp.where(core == 0, whole_conv[:, cols - 1], whole_conv[:, 0])
    for c in cp_vec:
        c.wait()
    vec = [v[...].reshape(1, channels) for v in (v0, v1, v2, v3, v4, v5)]
    cp_snorm.wait()

    mark("barrier")
    pl.semaphore_wait(barrier, patches - 1)
    mark("sends")
    send_stats(0)
    edge_copy(1, 0).start()

    @pl.when(jnp.logical_not(row_last))
    def _():
        halo_copy(0, 1).start()
        edge_copy(0, 1).start()

    @pl.when(jnp.logical_not(row_first))
    def _():
        halo_copy(1, -1).start()
        edge_copy(2, -1).start()

    x_copy(me, index(zo, 1 - yi, core), xy_send.at[0]).start()

    def z_send(d, carry):
        x_copy(me, index(lax.rem(zo + d, outer), yi, core), xz_send.at[d]).start()
        return carry

    lax.fori_loop(1, outer, z_send, 0)
    x_copy(me, partner, xc_send.at[0]).start()

    def forward_z(d, carry):
        slot = index(lax.rem(zo - d + outer, outer), yi, core)
        x_copy(slot, partner, xz_send.at[d]).wait_recv()
        x_copy(slot, index(zo, 1 - yi, core), xy_send.at[d]).start()
        x_copy(slot, partner, xc_send.at[d]).start()
        return carry

    def forward_y(d, carry):
        slot = index(lax.rem(zo - d + outer, outer), 1 - yi, core)
        x_copy(slot, partner, xz_send.at[0]).wait_recv()
        x_copy(slot, partner, xc_send.at[outer + d]).start()
        return carry

    mark("text")
    cp_tk.wait()
    cp_tv.wait()
    for b in range(images):
        tk[b] = tk_in[:, b, :]
        tv[b] = tv_in[:, b, :]
    mark("wait0")
    table = finish_stats(0)
    mark("norm0")
    for b in range(images):
        v = normed(x, table, b, vec[0], vec[1])
        lhs[1, b * cols:(b + 1) * cols, :] = (v * (1.0 / (1.0 + jnp.exp(-v)))).astype(BF16)

    mark("halo_wait")
    edge_copy(1, 0).wait_recv()

    @pl.when(jnp.logical_not(row_first))
    def _():
        halo_copy(0, 1).wait_recv()
        edge_copy(0, 1).wait_recv()

    @pl.when(jnp.logical_not(row_last))
    def _():
        halo_copy(1, -1).wait_recv()
        edge_copy(2, -1).wait_recv()

    mark("lhs")
    for which, row in ((0, 0), (1, 2)):
        lhs[row, :rows, :] = halo[which].reshape(rows, channels)
    filler = jnp.zeros((lhs.shape[1] - rows - images, channels), F32)
    for row in range(3):
        lhs[row, rows:, :] = jnp.concatenate([edges[row], filler], axis=0).astype(BF16)

    mark("conv")
    third = [1 + (outer - 1) * t // 3 for t in range(4)]
    parts = []
    for j in range(3):
        mark(f"conv{j}")
        total = None
        for i in range(3):
            cp_wc[i, j].wait()
            term = dot(lhs[i], wc[i, j])
            total = term if total is None else total + term
        parts.append(total)
        if j < 2:
            mark(f"fwd{j}")
            lax.fori_loop(third[j], third[j + 1], forward_z, 0)
    mark("shift")
    place = lax.broadcasted_iota(jnp.int32, (cols, channels), 0)
    for b in range(images):
        left = pltpu.roll(parts[0][b * cols:(b + 1) * cols], 1, 0)
        right = pltpu.roll(parts[2][b * cols:(b + 1) * cols], cols - 1, 0)
        left_edge = jnp.where(core == 1, parts[0][rows + b:rows + b + 1], 0.0)
        right_edge = jnp.where(core == 0, parts[2][rows + b:rows + b + 1], 0.0)
        left = jnp.where(place == 0, left_edge, left)
        right = jnp.where(place == cols - 1, right_edge, right)
        conv = left + parts[1][b * cols:(b + 1) * cols] + right
        hid[b * cols:(b + 1) * cols, :] = x[b * cols:(b + 1) * cols] + conv + vec[2]

    mark("stats1")
    hidden = hid[...]
    local_stats(1, hidden)
    mark("send1")
    send_stats(1)
    lax.fori_loop(third[2], third[3], forward_z, 0)
    mark("fwd_y")
    lax.fori_loop(0, outer, forward_y, 0)

    def from_partner(t, carry):
        x_copy(t * 2 + (1 - core), partner, xz_send.at[0]).wait_recv()
        return carry

    mark("partner")
    lax.fori_loop(0, chips, from_partner, 0)
    mark("kv")
    cp_w[0].wait()
    cp_w[1].wait()
    span = patches * cols
    piece = min(span, 256)

    def stale_kv(t, carry):
        at = pl.ds(pl.multiple_of(t * piece, piece), piece)
        for b in range(images):
            block = xall[b, at, :]
            kall[b, at, :] = dot(block, ws[0]).astype(BF16)
            vall[b, at, :] = dot(block, ws[1]).astype(BF16)
        return carry

    lax.fori_loop(0, span // piece, stale_kv, 0)
    mark("wait1")
    cp_w[2].wait()
    table = finish_stats(1)
    mark("norm1")
    attn_in = jnp.concatenate(
        [normed(hidden, table, b, vec[3], vec[4]) for b in range(images)], axis=0
    ).astype(BF16)
    own = pl.ds(pl.multiple_of(me * cols, cols), cols)
    fresh_k = dot(attn_in, ws[0]).astype(BF16)
    fresh_v = dot(attn_in, ws[1]).astype(BF16)
    for b in range(images):
        kall[b, own, :] = fresh_k[b * cols:(b + 1) * cols]
        vall[b, own, :] = fresh_v[b * cols:(b + 1) * cols]
    mark("q")
    scale = HEAD_DIM ** -0.5
    lane = lax.broadcasted_iota(jnp.int32, (cols, LANES), 1)

    def heads(q, keys, values):
        for b in range(images):
            for pair in range(channels // LANES):
                at = slice(pair * LANES, (pair + 1) * LANES)
                part = pair_attention(
                    q[b * cols:(b + 1) * cols, at], keys[b, :, at], values[b, :, at], lane
                )
                att[b * cols:(b + 1) * cols, at] = part.astype(BF16)

    heads(dot(attn_in, ws[2]).astype(BF16).astype(F32) * scale, kall, vall)
    mark("out_ln")
    cp_w[3].wait()
    mixed = hidden + dot(att[...], ws[3])
    centred = mixed - jnp.mean(mixed, axis=-1, keepdims=True)
    variance = jnp.mean(centred * centred, axis=-1, keepdims=True)
    layer_in = (centred * lax.rsqrt(variance + EPSILON) * vec[5]).astype(BF16)
    mark("cross")
    cp_w[4].wait()
    heads(dot(layer_in, ws[4]).astype(BF16).astype(F32) * scale, tk, tv)
    att_ref[...] = att[...]
    mixed_ref[...] = mixed

    mark("drain")
    def drain_stats(d, carry):
        stat_copy(0, me, d).wait_send()
        stat_copy(1, me, d).wait_send()
        return carry

    lax.fori_loop(1, patches, drain_stats, 0)

    def drain_z(d, carry):
        x_copy(me, partner, xz_send.at[d]).wait_send()
        return carry

    lax.fori_loop(1, outer, drain_z, 0)

    def drain_y(d, carry):
        x_copy(me, partner, xy_send.at[d]).wait_send()
        return carry

    lax.fori_loop(0, outer, drain_y, 0)

    def drain_c(d, carry):
        x_copy(me, partner, xc_send.at[d]).wait_send()
        return carry

    lax.fori_loop(0, chips, drain_c, 0)
    edge_copy(1, 0).wait_send()

    @pl.when(jnp.logical_not(row_last))
    def _():
        halo_copy(0, 1).wait_send()
        edge_copy(0, 1).wait_send()

    @pl.when(jnp.logical_not(row_first))
    def _():
        halo_copy(1, -1).wait_send()
        edge_copy(2, -1).wait_send()


def solution(mesh):
    patches = mesh.shape["patch"]

    def on_device(
        features, stale_conv_in, stale_normed, first_gain, first_bias, conv_weight, conv_bias,
        second_gain, second_bias, query_weight, key_weight, value_weight, output_weight,
        layer_gain, cross_query, cross_output, text_keys, text_values,
    ):
        images, _, cols, channels = features.shape
        rows = images * cols
        span = patches * cols
        outer = patches // 4
        ctx = text_keys.shape[1]

        def flat(a):
            return a.reshape(images, cols, channels)

        dma = pltpu.SemaphoreType.DMA
        mixed, attended = pl.pallas_call(
            functools.partial(kernel, patches, images, cols),
            out_shape=(
                jax.ShapeDtypeStruct((rows, channels), F32),
                jax.ShapeDtypeStruct((rows, channels), BF16),
            ),
            in_specs=[pl.BlockSpec(memory_space=pl.ANY)] * 17,
            out_specs=(pl.BlockSpec(memory_space=pltpu.VMEM),) * 2,
            scratch_shapes=[
                pltpu.VMEM((images, cols, channels), BF16),
                pltpu.VMEM((images, cols, channels), BF16),
                pltpu.VMEM((images, span, channels), BF16),
                pltpu.VMEM((images, span, channels), BF16),
                pltpu.VMEM((images, span, channels), BF16),
                pltpu.VMEM(conv_weight.shape, BF16),
                pltpu.VMEM((5, channels, channels), BF16),
                *[pltpu.VMEM((channels,), F32)] * 6,
                pltpu.VMEM((ctx, images, channels), BF16),
                pltpu.VMEM((ctx, images, channels), BF16),
                pltpu.VMEM((images, ctx, channels), BF16),
                pltpu.VMEM((images, ctx, channels), BF16),
                pltpu.VMEM((2, patches, 2 * images, LANES), F32),
                pltpu.VMEM((2, images, cols, channels), BF16),
                pltpu.VMEM((images, channels), F32),
                pltpu.VMEM((3, images, channels), F32),
                pltpu.VMEM((3, rows + 16, channels), BF16),
                pltpu.VMEM((rows, channels), F32),
                pltpu.VMEM((rows, channels), BF16),
                dma((2, patches)), dma((2, patches)),
                dma((outer,)), dma((outer,)), dma((2 * outer,)), dma((patches,)),
                dma((2,)), dma((2,)), dma((3,)), dma((3,)),
                dma((5,)), dma((9,)), dma((5,)), dma((6,)),
            ],
            compiler_params=pltpu.CompilerParams(
                collective_id=0, has_side_effects=True, vmem_limit_bytes=63000 * 1024
            ),
        )(
            flat(features), flat(stale_conv_in), flat(stale_normed), first_gain, first_bias,
            conv_weight, conv_bias, second_gain, second_bias, query_weight, key_weight,
            value_weight, output_weight, layer_gain, cross_query,
            text_keys.transpose(1, 0, 2), text_values.transpose(1, 0, 2),
        )
        return (mixed + dot(attended, cross_output)).reshape(features.shape)

    act = P("grp", "patch", None, None)
    text = P("grp", None, None)
    return jax.shard_map(
        on_device, mesh=mesh,
        in_specs=(act,) * 3 + (P(),) * 13 + (text,) * 2,
        out_specs=act, check_vma=False,
    )
```
